32 devices in a mesh: rows: 4 (over z), cols: 4 (over x, core), rep: 2 (over y).
Axes of the slice: x: 2, y: 2, z: 4, core: 2. Of those that a mesh axis runs over, the one named last changes fastest.
Arguments:
- matrix: float32 [16384, 8192], P(('rep', 'rows'), 'cols'), parts along dimension 0, may hold values from -0.0625 to 0.0625
- labels: int32 [16384], P(('rep', 'rows')), parts along dimension 0, may hold values from 0 to 1
- lambdas: float32 [64], P('rep'), parts along dimension 0, may hold values from 0.01 to 0.2
- x_prev: float32 [64, 8192], P('rep', 'cols'), parts along dimension 0, may hold values from -4 to 4
- w_prev: float32 [64, 8192], P('rep', 'cols'), parts along dimension 0, may hold values from -4 to 4
- p_prev: float32 [64, 8192], P('rep', 'cols'), parts along dimension 0, may hold values from -1.5 to 1.5
- z_prev: float32 [64, 8192], P('rep', 'rows'), parts along dimension 0, may hold values from -6 to 6
- u_prev: float32 [64, 8192], P('rep', 'rows'), parts along dimension 0, may hold values from -6 to 6
Outputs:
- coeffs: float32 [64, 8192], P('rep', 'cols'), parts along dimension 0
- sparse: float32 [64, 8192], P('rep', 'cols'), parts along dimension 0
- margins: float32 [64, 8192], P('rep', 'rows'), parts along dimension 0
- margin_dual: float32 [64, 8192], P('rep', 'rows'), parts along dimension 0
The draws below stay inside these ranges and needn't reach their ends.
There are 2 independent parts, one for each index of `rep`. The reference program is written for one: setup_inputs(seed, part) draws one part's arguments, and reference() takes and returns one part's arrays. A program takes and returns all parts, laid end to end along the dimension named above; each array names one. Nothing has to cross between parts.
All inputs are finite; a program needn't handle non-finite values.
Results may differ from the reference program's by a relative error of at most 0.0003.
Values sent between devices are 32-bit elements; how exact they have to be, the bound alone decides.
A program may use at most 128 MiB of HBM per device.

```python
import math
import jax
import jax.numpy as jnp
from jax import lax

FEATURES = 8192
PATHS = 32
ITERS = 2
CG_STEPS = 5
NEWTON_STEPS = 8
SAMPLES = 8192


def touch_ends(result, key, smallest, largest):
    longest = result.shape.index(max(result.shape))
    spots = []
    for shift in (0, 1):
        where = [jax.random.randint(jax.random.fold_in(key, axis), (), 0, length) for axis, length in enumerate(result.shape)]
        where[longest] = (where[longest] + shift) % result.shape[longest]
        spots.append(tuple(where))
    return result.at[spots[0]].set(smallest).at[spots[1]].set(largest)


def shard_levels(stream_key, extent, cuts, least, top_value):
    def one(position, shards_of):
        steps = jax.random.uniform(jax.random.fold_in(jax.random.fold_in(stream_key, 6), position), (shards_of,), jnp.float32, least / len(cuts), top_value / len(cuts))
        return jnp.repeat(jnp.exp(steps), extent[position] // shards_of).reshape((-1,) + (1,) * (len(extent) - position - 1))

    gain = one(*cuts[0])
    for cut in cuts[1:]:
        gain = gain * one(*cut)
    return gain


def gaussian(rng, extent, scale, bound, pieces=(), held_as=jnp.bfloat16):
    loudness = shard_levels(rng, extent, pieces, -0.22, 0.18) if pieces else 1.0
    result = jax.random.normal(rng, extent, jnp.float32) * scale * loudness
    return jnp.minimum(jnp.maximum(result, -bound), bound).astype(held_as)


def setup_inputs(seed: int = 0, part: int = 0) -> dict:
    key_of = jax.random.split(jax.random.key(seed), 9)
    own_keys = jax.random.split(jax.random.fold_in(key_of[8], part), 9)
    matrix = gaussian(own_keys[0], (SAMPLES, FEATURES), FEATURES ** -0.5, 0.0625, ((0, 4), (1, 4)), jnp.float32)
    labels = touch_ends(jax.random.randint(own_keys[1], (SAMPLES,), 0, 2), jax.random.fold_in(own_keys[1], 1), 0, 1).astype(jnp.int32)
    lambdas = jnp.clip(jnp.exp(jax.random.uniform(own_keys[2], (PATHS,), jnp.float32, math.log(0.01), math.log(0.2))), 0.01, 0.2)
    x_prev = gaussian(own_keys[3], (PATHS, FEATURES), 0.3, 4.0, ((1, 4),), jnp.float32)
    w_prev = gaussian(own_keys[4], (PATHS, FEATURES), 0.3, 4.0, ((1, 4),), jnp.float32)
    p_prev = gaussian(own_keys[5], (PATHS, FEATURES), 0.1, 1.5, ((1, 4),), jnp.float32)
    z_prev = gaussian(own_keys[6], (PATHS, SAMPLES), 1.0, 6.0, ((1, 4),), jnp.float32)
    u_prev = gaussian(own_keys[7], (PATHS, SAMPLES), 0.5, 6.0, ((1, 4),), jnp.float32)
    return {"matrix": matrix, "labels": labels, "lambdas": lambdas, "x_prev": x_prev, "w_prev": w_prev, "p_prev": p_prev, "z_prev": z_prev, "u_prev": u_prev}


HIGH = lax.Precision.HIGHEST


def apply_rows(vec, matrix):
    return lax.dot_general(vec, matrix, (((1,), (1,)), ((), ())), precision=HIGH, preferred_element_type=jnp.float32)


def apply_cols(vec, matrix):
    return lax.dot_general(vec, matrix, (((1,), (0,)), ((), ())), precision=HIGH, preferred_element_type=jnp.float32)


def proximal(target, sign):
    margin = target
    for step in range(NEWTON_STEPS):
        grad = margin - target - sign * jax.nn.sigmoid(-sign * margin)
        hess = 1.0 + jax.nn.sigmoid(margin) * jax.nn.sigmoid(-margin)
        margin = margin - grad / hess
    return margin


def reference(matrix, labels, lambdas, x_prev, w_prev, p_prev, z_prev, u_prev):
    sign = 2.0 * labels.astype(jnp.float32) - 1.0
    coeffs, sparse, dual, margins, margin_dual = x_prev, w_prev, p_prev, z_prev, u_prev
    for outer in range(ITERS):
        resid = (sparse - dual - coeffs) + apply_cols(margins - margin_dual - apply_rows(coeffs, matrix), matrix)
        direction = resid
        norm_now = jnp.sum(resid * resid, axis=1)
        for step in range(CG_STEPS):
            image = direction + apply_cols(apply_rows(direction, matrix), matrix)
            alpha = norm_now / jnp.sum(direction * image, axis=1)
            coeffs = coeffs + alpha[:, None] * direction
            resid = resid - alpha[:, None] * image
            if step + 1 < CG_STEPS:
                norm_next = jnp.sum(resid * resid, axis=1)
                direction = resid + (norm_next / norm_now)[:, None] * direction
                norm_now = norm_next
        target = apply_rows(coeffs, matrix) + margin_dual
        margins = proximal(target, sign[None, :])
        margin_dual = target - margins
        total = coeffs + dual
        sparse = jnp.sign(total) * jnp.maximum(jnp.abs(total) - lambdas[:, None], 0.0)
        dual = total - sparse
    return coeffs, sparse, margins, margin_dual
```

```python
import functools

import jax
import jax.numpy as jnp
from jax import lax
from jax.experimental import pallas as pl
from jax.experimental.pallas import tpu as pltpu
from jax.sharding import PartitionSpec as P

ITERS = 2
CG_STEPS = 5
NEWTON_STEPS = 8
TILE = 256
F32 = jnp.float32
BF16 = jnp.bfloat16
MESH = pl.DeviceIdType.MESH


def split(value):
    hi = value.astype(BF16)
    return hi, (value - hi.astype(F32)).astype(BF16)


class Group:
    def __init__(self, axis, n, part, land, full, note, notes, sems):
        self.axis, self.n = axis, n
        self.part, self.land, self.full, self.note, self.notes = part, land, full, note, notes
        self.send, self.recv = sems
        self.me = lax.axis_index(axis)
        self.width = part.shape[2]

    def peer(self, o):
        return lax.rem(self.me + 1 + o, self.n)

    def copy(self, kind, o, src, dst):
        return pltpu.make_async_remote_copy(
            src_ref=src,
            dst_ref=dst,
            send_sem=self.send.at[kind, o],
            recv_sem=self.recv.at[kind, o],
            device_id={self.axis: self.peer(o)},
            device_id_type=MESH,
        )

    def scatter(self, o):
        return self.copy(0, o, self.part.at[self.peer(o)], self.land.at[o])

    def gather(self, o):
        return self.copy(1, o, self.full.at[self.me], self.full.at[self.me])

    def tell(self, o):
        return self.copy(2, o, self.note, self.notes.at[o])

    def start_notes(self, value):
        self.note[...] = value
        for o in range(self.n - 1):
            self.tell(o).start()

    def finish_notes(self):
        total = self.note[...]
        for o in range(self.n - 1):
            self.tell(o).wait_recv()
            total = total + self.notes[o]
        for o in range(self.n - 1):
            self.tell(o).wait_send()
        return total

    def multiply(self, both, hi_ref, lo_ref):
        paths = both.shape[0] // 2
        step = min(TILE, self.width)

        def chunk(o, carry):
            owner = self.peer(o)
            for t in range(self.width // step):
                cols = pl.ds(pl.multiple_of(owner * self.width + t * step, 128), step)
                wide = jnp.dot(both[...], hi_ref[:, cols], preferred_element_type=F32)
                low = jnp.dot(both[0:paths, :], lo_ref[:, cols], preferred_element_type=F32)
                self.part[owner, :, t * step : (t + 1) * step] = wide[:paths] + wide[paths:] + low

            @pl.when(o < self.n - 1)
            def _():
                self.scatter(o).start()

            return carry

        lax.fori_loop(0, self.n, chunk, 0)

    def finish_sum(self):
        total = self.part[self.me]
        for o in range(self.n - 1):
            self.scatter(o).wait_recv()
            total = total + self.land[o]
        self.full[self.me] = total
        for o in range(self.n - 1):
            self.gather(o).start()
        for o in range(self.n - 1):
            self.scatter(o).wait_send()
        for o in range(self.n - 1):
            self.gather(o).wait()


def kernel(
    nc, nr, matrix, sign, lambdas, x_prev, w_prev, p_prev, z_prev, u_prev,
    coeffs, sparse, margins, mdual,
    a_hi, a_lo, t_hi, t_lo, stage, stage_sem, both_f, both_s,
    dual, resid, direction, image_of, mapped, scal,
    c_part, c_land, c_full, c_note, c_notes, c_send, c_recv,
    r_part, r_land, r_full, r_note, r_notes, r_send, r_recv,
):
    cols = Group("cols", nc, c_part, c_land, c_full, c_note, c_notes, (c_send, c_recv))
    rows = Group("rows", nr, r_part, r_land, r_full, r_note, r_notes, (r_send, r_recv))
    samples, features = matrix.shape
    paths = x_prev.shape[0]
    blocks = samples // TILE

    barrier = pltpu.get_barrier_semaphore()
    for group in (cols, rows):
        for o in range(group.n - 1):
            pl.semaphore_signal(
                barrier, inc=1, device_id={group.axis: group.peer(o)}, device_id_type=MESH
            )

    def load(i, slot):
        return pltpu.make_async_copy(
            matrix.at[pl.ds(pl.multiple_of(i * TILE, TILE), TILE)], stage.at[slot], stage_sem.at[slot]
        )

    load(0, 0).start()
    coeffs[...] = x_prev[...]
    sparse[...] = w_prev[...]
    dual[...] = p_prev[...]
    margins[...] = z_prev[...]
    mdual[...] = u_prev[...]
    resid[...] = x_prev[...]
    direction[...] = jnp.zeros_like(direction)
    mapped[...] = jnp.zeros_like(mapped)
    image_of[...] = jnp.zeros_like(image_of)
    scal[...] = jnp.ones_like(scal)
    lane = lax.broadcasted_iota(jnp.int32, (paths, 128), 1)

    def prepare(i, carry):
        slot = lax.rem(i, 2)
        load(i, slot).wait()

        @pl.when(i + 1 < blocks)
        def _():
            load(i + 1, 1 - slot).start()

        down = pl.ds(pl.multiple_of(i * TILE, TILE), TILE)

        def block(j, carry):
            across = pl.ds(pl.multiple_of(j * TILE, TILE), TILE)
            value = stage[slot, :, across]
            a_hi[down, across], a_lo[down, across] = split(value)
            t_hi[across, down], t_lo[across, down] = split(value.T)
            return carry

        return lax.fori_loop(0, features // TILE, block, carry)

    lax.fori_loop(0, blocks, prepare, 0)
    pl.semaphore_wait(barrier, cols.n + rows.n - 2)

    def spread(value):
        return jnp.broadcast_to(value, (paths, 128))

    def rowsum(value):
        return jnp.sum(value, axis=1, keepdims=True)

    def advance(alpha):
        coeffs[...] += alpha * direction[...]
        image_of[...] += alpha * mapped[...]

    def proximal():
        for c in range(cols.n):
            at = slice(c * cols.width, (c + 1) * cols.width)
            target = image_of[:, at] + mdual[:, at]
            sgn = sign[:, at]

            def newton(_, m):
                s = 1.0 / (1.0 + jnp.exp(sgn * m))
                return m - (m - target - sgn * s) / (1.0 + s * (1.0 - s))

            m = lax.fori_loop(0, NEWTON_STEPS, newton, target)
            margins[:, at] = m
            mdual[:, at] = target - m
        total = coeffs[...] + dual[...]
        lam = lambdas[...]
        clipped = jnp.minimum(jnp.maximum(total, -lam), lam)
        sparse[...] = total - clipped
        dual[...] = clipped

    last = ITERS * CG_STEPS

    def pair(k, carry):
        step = lax.rem(k + CG_STEPS - 1, CG_STEPS)
        first = jnp.logical_or(step == 0, k == 0)
        closing = jnp.logical_or(step == CG_STEPS - 1, k == 0)
        r = resid[...]
        both_f[0:paths, :], both_f[paths:, :] = split(r)
        rr, rd = rowsum(r * r), rowsum(r * direction[...])
        cols.start_notes(jnp.where(lane == 0, rr, rd))
        cols.multiply(both_f, t_hi, t_lo)
        notes = cols.finish_notes()
        rr, rd = spread(notes[:, 0:1]), spread(notes[:, 1:2])
        beta = jnp.where(first, 0.0, rr / scal[0])
        scal[1] = rr + 2.0 * beta * rd + beta * beta * scal[1]
        scal[0] = rr
        beta = beta[:, 0:1]
        cols.finish_sum()

        @pl.when(k == 0)
        def _():
            for c in range(cols.n):
                image_of[:, c * cols.width : (c + 1) * cols.width] = cols.full[c]

        @pl.when(k > 0)
        def _():
            direction[...] = resid[...] + beta * direction[...]
            for c in range(cols.n):
                at = slice(c * cols.width, (c + 1) * cols.width)
                mapped[:, at] = cols.full[c] + beta * mapped[:, at]

        m = mapped[...]
        rows.start_notes(spread(rowsum(m * m)))

        @pl.when(closing)
        def _():
            @pl.when(k > 0)
            def _():
                sq = rows.finish_notes()
                advance((scal[0] / (scal[1] + sq))[:, 0:1])
                proximal()
                direction[...] = jnp.zeros_like(direction)
                mapped[...] = jnp.zeros_like(mapped)

            @pl.when(k == 0)
            def _():
                rows.finish_notes()

            both_s[0:paths, :], both_s[paths:, :] = split(margins[...] - mdual[...] - image_of[...])

        @pl.when(jnp.logical_not(closing))
        def _():
            both_s[0:paths, :], both_s[paths:, :] = split(m)

        @pl.when(k < last)
        def _():
            rows.multiply(both_s, a_hi, a_lo)

            @pl.when(jnp.logical_not(closing))
            def _():
                sq = rows.finish_notes()
                alpha = scal[0] / (scal[1] + sq)
                scal[2] = alpha
                advance(alpha[:, 0:1])

            rows.finish_sum()

            @pl.when(closing)
            def _():
                for c in range(rows.n):
                    at = slice(c * rows.width, (c + 1) * rows.width)
                    resid[:, at] = sparse[:, at] - dual[:, at] - coeffs[:, at] + rows.full[c]

            @pl.when(jnp.logical_not(closing))
            def _():
                alpha = scal[2][:, 0:1]
                for c in range(rows.n):
                    at = slice(c * rows.width, (c + 1) * rows.width)
                    resid[:, at] = resid[:, at] - alpha * (direction[:, at] + rows.full[c])

        return carry

    lax.fori_loop(0, last + 1, pair, 0)


def local(nc, nr, matrix, labels, lambdas, x_prev, w_prev, p_prev, z_prev, u_prev):
    sign = (2.0 * labels.astype(F32) - 1.0)[None, :]
    samples, features = matrix.shape
    paths = x_prev.shape[0]
    fvec, svec = (paths, features), (paths, samples)

    def comm(n, length):
        width = length // n
        return [
            pltpu.VMEM((n, paths, width), F32),
            pltpu.VMEM((n - 1, paths, width), F32),
            pltpu.VMEM((n, paths, width), F32),
            pltpu.VMEM((paths, 128), F32),
            pltpu.VMEM((n - 1, paths, 128), F32),
            pltpu.SemaphoreType.DMA((3, n - 1)),
            pltpu.SemaphoreType.DMA((3, n - 1)),
        ]

    vmem = pl.BlockSpec(memory_space=pltpu.VMEM)
    return pl.pallas_call(
        functools.partial(kernel, nc, nr),
        out_shape=tuple(jax.ShapeDtypeStruct(s, F32) for s in (fvec, fvec, svec, svec)),
        in_specs=[pl.BlockSpec(memory_space=pl.ANY)] + [vmem] * 7,
        out_specs=(vmem,) * 4,
        scratch_shapes=[
            pltpu.VMEM((samples, features), BF16),
            pltpu.VMEM((samples, features), BF16),
            pltpu.VMEM((features, samples), BF16),
            pltpu.VMEM((features, samples), BF16),
            pltpu.VMEM((2, TILE, features), F32),
            pltpu.SemaphoreType.DMA((2,)),
            pltpu.VMEM((2 * paths, features), BF16),
            pltpu.VMEM((2 * paths, samples), BF16),
            pltpu.VMEM(fvec, F32),
            pltpu.VMEM(fvec, F32),
            pltpu.VMEM(fvec, F32),
            pltpu.VMEM(svec, F32),
            pltpu.VMEM(svec, F32),
            pltpu.VMEM((3, paths, 128), F32),
        ]
        + comm(nc, samples)
        + comm(nr, features),
        compiler_params=pltpu.CompilerParams(
            collective_id=0, has_side_effects=True, vmem_limit_bytes=60 * 1024 * 1024
        ),
    )(matrix, sign, lambdas[:, None], x_prev, w_prev, p_prev, z_prev, u_prev)


def solution(mesh):
    return jax.shard_map(
        functools.partial(local, mesh.shape["cols"], mesh.shape["rows"]),
        mesh=mesh,
        in_specs=(
            P(("rep", "rows"), "cols"),
            P(("rep", "rows")),
            P("rep"),
            P("rep", "cols"),
            P("rep", "cols"),
            P("rep", "cols"),
            P("rep", "rows"),
            P("rep", "rows"),
        ),
        out_specs=(P("rep", "cols"), P("rep", "cols"), P("rep", "rows"), P("rep", "rows")),
        check_vma=False,
    )
```

```python
import functools

import jax
import jax.numpy as jnp
from jax import lax
from jax.experimental import pallas as pl
from jax.experimental.pallas import tpu as pltpu
from jax.sharding import PartitionSpec as P

ITERS = 2
CG_STEPS = 5
NEWTON_STEPS = 8
TILE = 256
LAG = 3
F32 = jnp.float32
BF16 = jnp.bfloat16
MESH = pl.DeviceIdType.MESH


def split(value):
    hi = value.astype(BF16)
    return hi, (value - hi.astype(F32)).astype(BF16)


class Group:
    def __init__(self, axis, n, part, land, full, note, notes, send, recv, tell_send, tell_recv):
        self.axis, self.n = axis, n
        self.part, self.land, self.full, self.note, self.notes = part, land, full, note, notes
        self.send, self.recv = send, recv
        self.tell_send, self.tell_recv = tell_send, tell_recv
        self.me = lax.axis_index(axis)
        self.count, self.paths, self.width = part.shape

    @staticmethod
    def shape(n, length):
        return (n, n - 1, length // n)

    def peer(self, o):
        return lax.rem(self.me + 1 + o, self.n)

    def copy(self, kind, o, src, dst, peer):
        return pltpu.make_async_remote_copy(
            src_ref=src,
            dst_ref=dst,
            send_sem=self.send.at[kind, o],
            recv_sem=self.recv.at[kind, o],
            device_id={self.axis: peer},
            device_id_type=MESH,
        )

    def scatter(self, o):
        peer = self.peer(o)
        return self.copy(0, o, self.part.at[peer], self.land.at[0, o], peer)

    def gather(self, o):
        return self.copy(1, o, self.full.at[self.me], self.full.at[self.me], self.peer(o))

    def tell(self, turn, o):
        return pltpu.make_async_remote_copy(
            src_ref=self.note.at[turn],
            dst_ref=self.notes.at[turn, o],
            send_sem=self.tell_send.at[turn, o],
            recv_sem=self.tell_recv.at[turn, o],
            device_id={self.axis: self.peer(o)},
            device_id_type=MESH,
        )

    def start_notes(self, turn, value):
        self.note[turn] = value
        for o in range(self.n - 1):
            self.tell(turn, o).start()

    def finish_notes(self, turn):
        for o in range(self.n - 1):
            self.tell(turn, o).wait()
        total = jnp.zeros(self.note.shape[1:], F32)
        for d in range(self.n):
            term = self.note[turn]
            for o in range(self.n - 1):
                term = jnp.where(self.peer(self.n - 2 - o) == d, self.notes[turn, o], term)
            total = total + term
        return total

    def product(self, both, hi_ref, lo_ref, owner):
        paths, step = self.paths, min(TILE, self.width)
        for t in range(self.width // step):
            cols = pl.ds(pl.multiple_of(owner * self.width + t * step, 128), step)
            wide = jnp.dot(both[...], hi_ref[:, cols], preferred_element_type=F32)
            low = jnp.dot(both[0:paths, :], lo_ref[:, cols], preferred_element_type=F32)
            self.part[owner, :, t * step : (t + 1) * step] = wide[:paths] + wide[paths:] + low

    def multiply(self, both, hi_ref, lo_ref, between=None):
        def chunk(o, carry):
            self.product(both, hi_ref, lo_ref, self.peer(o))

            @pl.when(o < self.n - 1)
            def _():
                self.scatter(o).start()

            return carry

        lax.fori_loop(0, self.n, chunk, 0)
        if between is not None:
            between()

    def finish_sum(self):
        total = self.part[self.me]
        for o in range(self.n - 1):
            self.scatter(o).wait_recv()
            total = total + self.land[0, o]
        self.full[self.me] = total
        for o in range(self.n - 1):
            self.gather(o).start()
        for o in range(self.n - 1):
            self.scatter(o).wait_send()
        for o in range(self.n - 1):
            self.gather(o).wait()


class Pairs(Group):
    @staticmethod
    def shape(n, length):
        return (length // TILE, length // TILE, TILE)

    def partner(self):
        return self.me + 1 - 2 * lax.rem(self.me, 2)

    def near(self, o, src):
        return self.copy(0, o, self.part.at[src], self.land.at[0, o], self.partner())

    def far(self, o, src):
        return self.copy(1, o, self.part.at[src], self.land.at[1, o], self.across())

    def back(self, o, src):
        return self.copy(2, o, self.full.at[src], self.full.at[src], self.partner())


class Square(Pairs):
    def across(self):
        return lax.rem(self.me + 2, 4)

    def multiply(self, both, hi_ref, lo_ref, between=None):
        half = self.count // 2
        core = lax.rem(self.me, 2)
        mine, other = core * half, (1 - core) * half

        def give(o, carry):
            self.product(both, hi_ref, lo_ref, other + o)
            self.near(o, other + o).start()
            return carry

        def keep(o, carry):
            self.product(both, hi_ref, lo_ref, mine + o)
            self.near(o, other + o).wait_recv()
            self.part[mine + o] += self.land[0, o]
            self.far(o, mine + o).start()
            return carry

        lax.fori_loop(0, half, give, 0)
        if between is not None:
            between()
        lax.fori_loop(0, half, keep, 0)

    def finish_sum(self):
        half = self.count // 2
        core = lax.rem(self.me, 2)
        mine, other = core * half, (1 - core) * half

        def total(o, carry):
            self.far(o, mine + o).wait_recv()
            self.full[mine + o] = self.part[mine + o] + self.land[1, o]
            self.back(o, mine + o).start()
            return carry

        def settle(o, carry):
            self.near(o, other + o).wait_send()
            self.far(o, mine + o).wait_send()
            self.back(o, mine + o).wait()
            return carry

        lax.fori_loop(0, half, total, 0)
        lax.fori_loop(0, half, settle, 0)


class Chain(Pairs):
    def across(self):
        return 3 - self.me

    def inner(self):
        return jnp.logical_or(self.me == 1, self.me == 2)

    def multiply(self, both, hi_ref, lo_ref, between=None):
        def chunk(o, carry):
            self.product(both, hi_ref, lo_ref, o)

            @pl.when(jnp.logical_not(self.inner()))
            def _():
                self.near(o, o).start()

            return carry

        lax.fori_loop(0, self.count, chunk, 0)
        if between is not None:
            between()

    def finish_sum(self):
        count = self.count

        @pl.when(self.inner())
        def _():
            def relay(o, carry):
                @pl.when(o < count)
                def _():
                    self.near(o, o).wait_recv()
                    self.part[o] += self.land[0, o]
                    self.far(o, o).start()

                @pl.when(o >= LAG)
                def _():
                    p = o - LAG
                    self.far(p, p).wait_recv()
                    self.full[p] = self.part[p] + self.land[1, p]
                    self.back(p, p).start()

                return carry

            def settle(o, carry):
                self.far(o, o).wait_send()
                self.back(o, o).wait_send()
                return carry

            lax.fori_loop(0, count + LAG, relay, 0)
            lax.fori_loop(0, count, settle, 0)

        @pl.when(jnp.logical_not(self.inner()))
        def _():
            def settle(o, carry):
                self.near(o, o).wait_send()
                self.back(o, o).wait_recv()
                return carry

            lax.fori_loop(0, count, settle, 0)


def col_kind(n):
    return Square if n == 4 else Group


def row_kind(n):
    return Chain if n == 4 else Group


def kernel(
    nc, nr, matrix, sign, lambdas, x_prev, w_prev, p_prev, z_prev, u_prev,
    coeffs, sparse, margins, mdual,
    a_hi, a_lo, t_hi, t_lo, stage, stage_sem, both_f, both_s,
    dual, resid, direction, image_of, mapped, scal,
    *comm,
):
    cols = col_kind(nc)("cols", nc, *comm[:9])
    rows = row_kind(nr)("rows", nr, *comm[9:])
    samples, features = matrix.shape
    paths = x_prev.shape[0]
    blocks = samples // TILE

    barrier = pltpu.get_barrier_semaphore()
    for group in (cols, rows):
        for o in range(group.n - 1):
            pl.semaphore_signal(
                barrier, inc=1, device_id={group.axis: group.peer(o)}, device_id_type=MESH
            )

    def load(i, slot):
        return pltpu.make_async_copy(
            matrix.at[pl.ds(pl.multiple_of(i * TILE, TILE), TILE)], stage.at[slot], stage_sem.at[slot]
        )

    load(0, 0).start()
    coeffs[...] = x_prev[...]
    sparse[...] = w_prev[...]
    dual[...] = p_prev[...]
    margins[...] = z_prev[...]
    mdual[...] = u_prev[...]
    resid[...] = x_prev[...]
    direction[...] = jnp.zeros_like(direction)
    mapped[...] = jnp.zeros_like(mapped)
    image_of[...] = jnp.zeros_like(image_of)
    scal[...] = jnp.ones_like(scal)
    lane = lax.broadcasted_iota(jnp.int32, (paths, 128), 1)

    def prepare(i, carry):
        slot = lax.rem(i, 2)
        load(i, slot).wait()

        @pl.when(i + 1 < blocks)
        def _():
            load(i + 1, 1 - slot).start()

        down = pl.ds(pl.multiple_of(i * TILE, TILE), TILE)

        def block(j, carry):
            across = pl.ds(pl.multiple_of(j * TILE, TILE), TILE)
            value = stage[slot, :, across]
            a_hi[down, across], a_lo[down, across] = split(value)
            t_hi[across, down], t_lo[across, down] = split(value.T)
            return carry

        return lax.fori_loop(0, features // TILE, block, carry)

    lax.fori_loop(0, blocks, prepare, 0)
    pl.semaphore_wait(barrier, cols.n + rows.n - 2)

    def spread(value):
        return jnp.broadcast_to(value, (paths, 128))

    def rowsum(value):
        return jnp.sum(value, axis=1, keepdims=True)

    def advance(alpha):
        coeffs[...] += alpha * direction[...]
        image_of[...] += alpha * mapped[...]

    def proximal():
        for c in range(cols.count):
            at = slice(c * cols.width, (c + 1) * cols.width)
            target = image_of[:, at] + mdual[:, at]
            sgn = sign[:, at]

            def newton(_, m):
                s = 1.0 / (1.0 + jnp.exp(sgn * m))
                return m - (m - target - sgn * s) / (1.0 + s * (1.0 - s))

            m = lax.fori_loop(0, NEWTON_STEPS, newton, target)
            margins[:, at] = m
            mdual[:, at] = target - m
        total = coeffs[...] + dual[...]
        lam = lambdas[...]
        clipped = jnp.minimum(jnp.maximum(total, -lam), lam)
        sparse[...] = total - clipped
        dual[...] = clipped

    last = ITERS * CG_STEPS

    def pair(k, carry):
        step = lax.rem(k + CG_STEPS - 1, CG_STEPS)
        first = jnp.logical_or(step == 0, k == 0)
        closing = jnp.logical_or(step == CG_STEPS - 1, k == 0)
        r = resid[...]
        both_f[0:paths, :], both_f[paths:, :] = split(r)
        rr, rd = rowsum(r * r), rowsum(r * direction[...])
        turn = lax.rem(k, 2)
        cols.start_notes(turn, jnp.where(lane == 0, rr, rd))

        def direction_step():
            notes = cols.finish_notes(turn)
            rr, rd = spread(notes[:, 0:1]), spread(notes[:, 1:2])
            beta = jnp.where(first, 0.0, rr / scal[0])
            scal[1] = rr + 2.0 * beta * rd + beta * beta * scal[1]
            scal[0] = rr
            scal[2] = beta

            @pl.when(k > 0)
            def _():
                direction[...] = resid[...] + beta[:, 0:1] * direction[...]

        cols.multiply(both_f, t_hi, t_lo, direction_step)
        cols.finish_sum()

        @pl.when(k == 0)
        def _():
            for c in range(cols.count):
                image_of[:, c * cols.width : (c + 1) * cols.width] = cols.full[c]

        @pl.when(k > 0)
        def _():
            beta = scal[2][:, 0:1]
            for c in range(cols.count):
                at = slice(c * cols.width, (c + 1) * cols.width)
                mapped[:, at] = cols.full[c] + beta * mapped[:, at]

        m = mapped[...]
        rows.start_notes(turn, spread(rowsum(m * m)))

        @pl.when(closing)
        def _():
            @pl.when(k > 0)
            def _():
                sq = rows.finish_notes(turn)
                advance((scal[0] / (scal[1] + sq))[:, 0:1])
                proximal()
                direction[...] = jnp.zeros_like(direction)
                mapped[...] = jnp.zeros_like(mapped)

            @pl.when(k == 0)
            def _():
                rows.finish_notes(turn)

            both_s[0:paths, :], both_s[paths:, :] = split(margins[...] - mdual[...] - image_of[...])

        @pl.when(jnp.logical_not(closing))
        def _():
            both_s[0:paths, :], both_s[paths:, :] = split(m)

        @pl.when(k < last)
        def _():
            def length_step():
                @pl.when(jnp.logical_not(closing))
                def _():
                    sq = rows.finish_notes(turn)
                    alpha = scal[0] / (scal[1] + sq)
                    scal[2] = alpha
                    advance(alpha[:, 0:1])

            rows.multiply(both_s, a_hi, a_lo, length_step)
            rows.finish_sum()

            @pl.when(closing)
            def _():
                for c in range(rows.count):
                    at = slice(c * rows.width, (c + 1) * rows.width)
                    resid[:, at] = sparse[:, at] - dual[:, at] - coeffs[:, at] + rows.full[c]

            @pl.when(jnp.logical_not(closing))
            def _():
                alpha = scal[2][:, 0:1]
                for c in range(rows.count):
                    at = slice(c * rows.width, (c + 1) * rows.width)
                    resid[:, at] = resid[:, at] - alpha * (direction[:, at] + rows.full[c])

        return carry

    lax.fori_loop(0, last + 1, pair, 0)


def local(nc, nr, matrix, labels, lambdas, x_prev, w_prev, p_prev, z_prev, u_prev):
    sign = (2.0 * labels.astype(F32) - 1.0)[None, :]
    samples, features = matrix.shape
    paths = x_prev.shape[0]
    fvec, svec = (paths, features), (paths, samples)

    def comm(kind, n, length):
        count, slots, width = kind.shape(n, length)
        return [
            pltpu.VMEM((count, paths, width), F32),
            pltpu.VMEM((2, slots, paths, width), F32),
            pltpu.VMEM((count, paths, width), F32),
            pltpu.VMEM((2, paths, 128), F32),
            pltpu.VMEM((2, n - 1, paths, 128), F32),
            pltpu.SemaphoreType.DMA((3, slots)),
            pltpu.SemaphoreType.DMA((3, slots)),
            pltpu.SemaphoreType.DMA((2, n - 1)),
            pltpu.SemaphoreType.DMA((2, n - 1)),
        ]

    vmem = pl.BlockSpec(memory_space=pltpu.VMEM)
    return pl.pallas_call(
        functools.partial(kernel, nc, nr),
        out_shape=tuple(jax.ShapeDtypeStruct(s, F32) for s in (fvec, fvec, svec, svec)),
        in_specs=[pl.BlockSpec(memory_space=pl.ANY)] + [vmem] * 7,
        out_specs=(vmem,) * 4,
        scratch_shapes=[
            pltpu.VMEM((samples, features), BF16),
            pltpu.VMEM((samples, features), BF16),
            pltpu.VMEM((features, samples), BF16),
            pltpu.VMEM((features, samples), BF16),
            pltpu.VMEM((2, TILE, features), F32),
            pltpu.SemaphoreType.DMA((2,)),
            pltpu.VMEM((2 * paths, features), BF16),
            pltpu.VMEM((2 * paths, samples), BF16),
            pltpu.VMEM(fvec, F32),
            pltpu.VMEM(fvec, F32),
            pltpu.VMEM(fvec, F32),
            pltpu.VMEM(svec, F32),
            pltpu.VMEM(svec, F32),
            pltpu.VMEM((3, paths, 128), F32),
        ]
        + comm(col_kind(nc), nc, samples)
        + comm(row_kind(nr), nr, features),
        compiler_params=pltpu.CompilerParams(
            collective_id=0, has_side_effects=True, vmem_limit_bytes=60 * 1024 * 1024
        ),
    )(matrix, sign, lambdas[:, None], x_prev, w_prev, p_prev, z_prev, u_prev)


def solution(mesh):
    return jax.shard_map(
        functools.partial(local, mesh.shape["cols"], mesh.shape["rows"]),
        mesh=mesh,
        in_specs=(
            P(("rep", "rows"), "cols"),
            P(("rep", "rows")),
            P("rep"),
            P("rep", "cols"),
            P("rep", "cols"),
            P("rep", "cols"),
            P("rep", "rows"),
            P("rep", "rows"),
        ),
        out_specs=(P("rep", "cols"), P("rep", "cols"), P("rep", "rows"), P("rep", "rows")),
        check_vma=False,
    )
```

```python
import functools

import jax
import jax.numpy as jnp
from jax import lax
from jax.experimental import pallas as pl
from jax.experimental.pallas import tpu as pltpu
from jax.sharding import PartitionSpec as P

ITERS = 2
CG_STEPS = 5
NEWTON_STEPS = 8
TILE = 256
CHUNK = 256
LAG = 3
F32 = jnp.float32
BF16 = jnp.bfloat16
MESH = pl.DeviceIdType.MESH


def split(value):
    hi = value.astype(BF16)
    return hi, (value - hi.astype(F32)).astype(BF16)


class Group:
    def __init__(self, axis, n, part, land, full, note, notes, send, recv, tell_send, tell_recv):
        self.axis, self.n = axis, n
        self.part, self.land, self.full, self.note, self.notes = part, land, full, note, notes
        self.send, self.recv = send, recv
        self.tell_send, self.tell_recv = tell_send, tell_recv
        self.me = lax.axis_index(axis)
        self.count, self.paths, self.width = part.shape

    @staticmethod
    def shape(n, length):
        return (n, n - 1, length // n)

    def peer(self, o):
        return lax.rem(self.me + 1 + o, self.n)

    def copy(self, kind, o, src, dst, peer):
        return pltpu.make_async_remote_copy(
            src_ref=src,
            dst_ref=dst,
            send_sem=self.send.at[kind, o],
            recv_sem=self.recv.at[kind, o],
            device_id={self.axis: peer},
            device_id_type=MESH,
        )

    def scatter(self, o):
        peer = self.peer(o)
        return self.copy(0, o, self.part.at[peer], self.land.at[0, o], peer)

    def gather(self, o):
        return self.copy(1, o, self.full.at[self.me], self.full.at[self.me], self.peer(o))

    def tell(self, turn, o):
        return pltpu.make_async_remote_copy(
            src_ref=self.note.at[turn],
            dst_ref=self.notes.at[turn, o],
            send_sem=self.tell_send.at[turn, o],
            recv_sem=self.tell_recv.at[turn, o],
            device_id={self.axis: self.peer(o)},
            device_id_type=MESH,
        )

    def start_notes(self, turn, *values):
        for i, value in enumerate(values):
            self.note[turn, i : i + 1, :] = value
        for o in range(self.n - 1):
            self.tell(turn, o).start()

    def finish_notes(self, turn):
        for o in range(self.n - 1):
            self.tell(turn, o).wait()
        total = jnp.zeros(self.note.shape[1:], F32)
        for d in range(self.n):
            term = self.note[turn]
            for o in range(self.n - 1):
                term = jnp.where(self.peer(self.n - 2 - o) == d, self.notes[turn, o], term)
            total = total + term
        return total

    def product(self, both, hi_ref, lo_ref, owner):
        paths, step = self.paths, min(CHUNK, self.width)
        for t in range(self.width // step):
            cols = pl.ds(pl.multiple_of(owner * self.width + t * step, 128), step)
            wide = jnp.dot(both[...], hi_ref[:, cols], preferred_element_type=F32)
            low = jnp.dot(both[0:paths, :], lo_ref[:, cols], preferred_element_type=F32)
            self.part[owner, :, t * step : (t + 1) * step] = wide[:paths] + wide[paths:] + low

    def multiply(self, both, hi_ref, lo_ref, between=None):
        def chunk(o, carry):
            self.product(both, hi_ref, lo_ref, self.peer(o))

            @pl.when(o < self.n - 1)
            def _():
                self.scatter(o).start()

            return carry

        lax.fori_loop(0, self.n, chunk, 0)
        if between is not None:
            between()

    def finish_sum(self):
        total = self.part[self.me]
        for o in range(self.n - 1):
            self.scatter(o).wait_recv()
            total = total + self.land[0, o]
        self.full[self.me] = total
        for o in range(self.n - 1):
            self.gather(o).start()
        for o in range(self.n - 1):
            self.scatter(o).wait_send()
        for o in range(self.n - 1):
            self.gather(o).wait()


class Pairs(Group):
    @staticmethod
    def shape(n, length):
        return (length // CHUNK, length // CHUNK, CHUNK)

    def partner(self):
        return self.me + 1 - 2 * lax.rem(self.me, 2)

    def near(self, o, src):
        return self.copy(0, o, self.part.at[src], self.land.at[0, o], self.partner())

    def far(self, o, src):
        return self.copy(1, o, self.part.at[src], self.land.at[1, o], self.across())

    def back(self, o, src):
        return self.copy(2, o, self.full.at[src], self.full.at[src], self.partner())


class Square(Pairs):
    def across(self):
        return lax.rem(self.me + 2, 4)

    def multiply(self, both, hi_ref, lo_ref, between=None):
        half = self.count // 2
        core = lax.rem(self.me, 2)
        mine, other = core * half, (1 - core) * half

        def give(o, carry):
            self.product(both, hi_ref, lo_ref, other + o)
            self.near(o, other + o).start()
            return carry

        def keep(o, carry):
            self.product(both, hi_ref, lo_ref, mine + o)
            self.near(o, other + o).wait_recv()
            self.part[mine + o] += self.land[0, o]
            self.far(o, mine + o).start()
            return carry

        lax.fori_loop(0, half, give, 0)
        if between is not None:
            between()
        lax.fori_loop(0, half, keep, 0)

    def finish_sum(self):
        half = self.count // 2
        core = lax.rem(self.me, 2)
        mine, other = core * half, (1 - core) * half

        def total(o, carry):
            self.far(o, mine + o).wait_recv()
            self.full[mine + o] = self.part[mine + o] + self.land[1, o]
            self.back(o, mine + o).start()
            return carry

        def settle(o, carry):
            self.near(o, other + o).wait_send()
            self.far(o, mine + o).wait_send()
            self.back(o, mine + o).wait()
            return carry

        lax.fori_loop(0, half, total, 0)
        lax.fori_loop(0, half, settle, 0)


class Chain(Pairs):
    def across(self):
        return 3 - self.me

    def inner(self):
        return jnp.logical_or(self.me == 1, self.me == 2)

    def multiply(self, both, hi_ref, lo_ref, between=None):
        def chunk(o, carry):
            self.product(both, hi_ref, lo_ref, o)

            @pl.when(jnp.logical_not(self.inner()))
            def _():
                self.near(o, o).start()

            return carry

        lax.fori_loop(0, self.count, chunk, 0)
        if between is not None:
            between()

    def finish_sum(self):
        count = self.count

        @pl.when(self.inner())
        def _():
            def relay(o, carry):
                @pl.when(o < count)
                def _():
                    self.near(o, o).wait_recv()
                    self.part[o] += self.land[0, o]
                    self.far(o, o).start()

                @pl.when(o >= LAG)
                def _():
                    p = o - LAG
                    self.far(p, p).wait_recv()
                    self.full[p] = self.part[p] + self.land[1, p]
                    self.back(p, p).start()

                return carry

            def settle(o, carry):
                self.far(o, o).wait_send()
                self.back(o, o).wait_send()
                return carry

            lax.fori_loop(0, count + LAG, relay, 0)
            lax.fori_loop(0, count, settle, 0)

        @pl.when(jnp.logical_not(self.inner()))
        def _():
            def settle(o, carry):
                self.near(o, o).wait_send()
                self.back(o, o).wait_recv()
                return carry

            lax.fori_loop(0, count, settle, 0)


def col_kind(n):
    return Square if n == 4 else Group


def row_kind(n):
    return Chain if n == 4 else Group


def kernel(
    nc, nr, matrix, sign, lambdas, x_prev, w_prev, p_prev, z_prev, u_prev,
    coeffs, sparse, margins, mdual,
    a_hi, a_lo, t_hi, t_lo, stage, stage_sem, both_f, both_s,
    dual, resid, direction, image_of, mapped, scal,
    *comm,
):
    cols = col_kind(nc)("cols", nc, *comm[:9])
    rows = row_kind(nr)("rows", nr, *comm[9:])
    samples, features = matrix.shape
    paths = x_prev.shape[0]
    blocks = samples // TILE

    barrier = pltpu.get_barrier_semaphore()
    for group in (cols, rows):
        for o in range(group.n - 1):
            pl.semaphore_signal(
                barrier, inc=1, device_id={group.axis: group.peer(o)}, device_id_type=MESH
            )

    def load(i, slot):
        return pltpu.make_async_copy(
            matrix.at[pl.ds(pl.multiple_of(i * TILE, TILE), TILE)], stage.at[slot], stage_sem.at[slot]
        )

    load(0, 0).start()
    coeffs[...] = x_prev[...]
    sparse[...] = w_prev[...]
    dual[...] = p_prev[...]
    margins[...] = z_prev[...]
    mdual[...] = u_prev[...]
    resid[...] = x_prev[...]
    direction[...] = jnp.zeros_like(direction)
    mapped[...] = jnp.zeros_like(mapped)
    image_of[...] = jnp.zeros_like(image_of)
    scal[...] = jnp.ones_like(scal)
    cols.note[...] = jnp.zeros_like(cols.note)
    rows.note[...] = jnp.zeros_like(rows.note)
    lane = lax.broadcasted_iota(jnp.int32, (paths, 128), 1)
    diagonal = lane == lax.broadcasted_iota(jnp.int32, (paths, 128), 0)

    def prepare(i, carry):
        slot = lax.rem(i, 2)
        load(i, slot).wait()

        @pl.when(i + 1 < blocks)
        def _():
            load(i + 1, 1 - slot).start()

        down = pl.ds(pl.multiple_of(i * TILE, TILE), TILE)

        def block(j, carry):
            across = pl.ds(pl.multiple_of(j * TILE, TILE), TILE)
            value = stage[slot, :, across]
            a_hi[down, across], a_lo[down, across] = split(value)
            t_hi[across, down], t_lo[across, down] = split(value.T)
            return carry

        return lax.fori_loop(0, features // TILE, block, carry)

    lax.fori_loop(0, blocks, prepare, 0)
    pl.semaphore_wait(barrier, cols.n + rows.n - 2)

    def spread(value):
        return jnp.broadcast_to(value, (paths, 128))

    def rowsum(value):
        value = jnp.sum(value, axis=1, keepdims=True)
        return jnp.sum(jnp.where(diagonal, value, 0.0), axis=0, keepdims=True)

    def per_path(row):
        return spread(jnp.sum(jnp.where(diagonal, row, 0.0), axis=1, keepdims=True))

    def advance(alpha):
        coeffs[...] += alpha * direction[...]
        image_of[...] += alpha * mapped[...]

    def proximal():
        for c in range(cols.count):
            at = slice(c * cols.width, (c + 1) * cols.width)
            target = image_of[:, at] + mdual[:, at]
            sgn = sign[:, at]

            def newton(_, m):
                s = 1.0 / (1.0 + jnp.exp(sgn * m))
                return m - (m - target - sgn * s) / (1.0 + s * (1.0 - s))

            m = lax.fori_loop(0, NEWTON_STEPS, newton, target)
            margins[:, at] = m
            mdual[:, at] = target - m
        total = coeffs[...] + dual[...]
        lam = lambdas[...]
        clipped = jnp.minimum(jnp.maximum(total, -lam), lam)
        sparse[...] = total - clipped
        dual[...] = clipped

    last = ITERS * CG_STEPS

    def pair(k, carry):
        step = lax.rem(k + CG_STEPS - 1, CG_STEPS)
        first = jnp.logical_or(step == 0, k == 0)
        closing = jnp.logical_or(step == CG_STEPS - 1, k == 0)
        r = resid[...]
        both_f[0:paths, :], both_f[paths:, :] = split(r)
        rr, rd = rowsum(r * r), rowsum(r * direction[...])
        turn = lax.rem(k, 2)
        cols.start_notes(turn, rr, rd)

        def direction_step():
            notes = cols.finish_notes(turn)
            rr, rd = per_path(notes[0:1]), per_path(notes[1:2])
            beta = jnp.where(first, 0.0, rr / scal[0])
            scal[1] = rr + 2.0 * beta * rd + beta * beta * scal[1]
            scal[0] = rr
            scal[2] = beta

            @pl.when(k > 0)
            def _():
                direction[...] = resid[...] + beta[:, 0:1] * direction[...]

        cols.multiply(both_f, t_hi, t_lo, direction_step)
        cols.finish_sum()

        @pl.when(k == 0)
        def _():
            for c in range(cols.count):
                image_of[:, c * cols.width : (c + 1) * cols.width] = cols.full[c]

        @pl.when(k > 0)
        def _():
            beta = scal[2][:, 0:1]
            for c in range(cols.count):
                at = slice(c * cols.width, (c + 1) * cols.width)
                mapped[:, at] = cols.full[c] + beta * mapped[:, at]

        m = mapped[...]
        rows.start_notes(turn, rowsum(m * m))

        @pl.when(closing)
        def _():
            @pl.when(k > 0)
            def _():
                sq = per_path(rows.finish_notes(turn)[0:1])
                advance((scal[0] / (scal[1] + sq))[:, 0:1])
                proximal()
                direction[...] = jnp.zeros_like(direction)
                mapped[...] = jnp.zeros_like(mapped)

            @pl.when(k == 0)
            def _():
                rows.finish_notes(turn)

            both_s[0:paths, :], both_s[paths:, :] = split(margins[...] - mdual[...] - image_of[...])

        @pl.when(jnp.logical_not(closing))
        def _():
            both_s[0:paths, :], both_s[paths:, :] = split(m)

        @pl.when(k < last)
        def _():
            def length_step():
                @pl.when(jnp.logical_not(closing))
                def _():
                    sq = per_path(rows.finish_notes(turn)[0:1])
                    alpha = scal[0] / (scal[1] + sq)
                    scal[2] = alpha
                    advance(alpha[:, 0:1])

            rows.multiply(both_s, a_hi, a_lo, length_step)
            rows.finish_sum()

            @pl.when(closing)
            def _():
                for c in range(rows.count):
                    at = slice(c * rows.width, (c + 1) * rows.width)
                    resid[:, at] = sparse[:, at] - dual[:, at] - coeffs[:, at] + rows.full[c]

            @pl.when(jnp.logical_not(closing))
            def _():
                alpha = scal[2][:, 0:1]
                for c in range(rows.count):
                    at = slice(c * rows.width, (c + 1) * rows.width)
                    resid[:, at] = resid[:, at] - alpha * (direction[:, at] + rows.full[c])

        return carry

    lax.fori_loop(0, last + 1, pair, 0)


def local(nc, nr, matrix, labels, lambdas, x_prev, w_prev, p_prev, z_prev, u_prev):
    sign = (2.0 * labels.astype(F32) - 1.0)[None, :]
    samples, features = matrix.shape
    paths = x_prev.shape[0]
    fvec, svec = (paths, features), (paths, samples)

    def comm(kind, n, length):
        count, slots, width = kind.shape(n, length)
        return [
            pltpu.VMEM((count, paths, width), F32),
            pltpu.VMEM((2, slots, paths, width), F32),
            pltpu.VMEM((count, paths, width), F32),
            pltpu.VMEM((2, 8, 128), F32),
            pltpu.VMEM((2, n - 1, 8, 128), F32),
            pltpu.SemaphoreType.DMA((3, slots)),
            pltpu.SemaphoreType.DMA((3, slots)),
            pltpu.SemaphoreType.DMA((2, n - 1)),
            pltpu.SemaphoreType.DMA((2, n - 1)),
        ]

    vmem = pl.BlockSpec(memory_space=pltpu.VMEM)
    return pl.pallas_call(
        functools.partial(kernel, nc, nr),
        out_shape=tuple(jax.ShapeDtypeStruct(s, F32) for s in (fvec, fvec, svec, svec)),
        in_specs=[pl.BlockSpec(memory_space=pl.ANY)] + [vmem] * 7,
        out_specs=(vmem,) * 4,
        scratch_shapes=[
            pltpu.VMEM((samples, features), BF16),
            pltpu.VMEM((samples, features), BF16),
            pltpu.VMEM((features, samples), BF16),
            pltpu.VMEM((features, samples), BF16),
            pltpu.VMEM((2, TILE, features), F32),
            pltpu.SemaphoreType.DMA((2,)),
            pltpu.VMEM((2 * paths, features), BF16),
            pltpu.VMEM((2 * paths, samples), BF16),
            pltpu.VMEM(fvec, F32),
            pltpu.VMEM(fvec, F32),
            pltpu.VMEM(fvec, F32),
            pltpu.VMEM(svec, F32),
            pltpu.VMEM(svec, F32),
            pltpu.VMEM((3, paths, 128), F32),
        ]
        + comm(col_kind(nc), nc, samples)
        + comm(row_kind(nr), nr, features),
        compiler_params=pltpu.CompilerParams(
            collective_id=0, has_side_effects=True, vmem_limit_bytes=60 * 1024 * 1024
        ),
    )(matrix, sign, lambdas[:, None], x_prev, w_prev, p_prev, z_prev, u_prev)


def solution(mesh):
    return jax.shard_map(
        functools.partial(local, mesh.shape["cols"], mesh.shape["rows"]),
        mesh=mesh,
        in_specs=(
            P(("rep", "rows"), "cols"),
            P(("rep", "rows")),
            P("rep"),
            P("rep", "cols"),
            P("rep", "cols"),
            P("rep", "cols"),
            P("rep", "rows"),
            P("rep", "rows"),
        ),
        out_specs=(P("rep", "cols"), P("rep", "cols"), P("rep", "rows"), P("rep", "rows")),
        check_vma=False,
    )
```

```python
import functools

import jax
import jax.numpy as jnp
from jax import lax
from jax.experimental import pallas as pl
from jax.experimental.pallas import tpu as pltpu
from jax.sharding import PartitionSpec as P

ITERS = 2
CG_STEPS = 5
NEWTON_STEPS = 8
TILE = 256
CHUNK = 256
LAG = 3
F32 = jnp.float32
BF16 = jnp.bfloat16
MESH = pl.DeviceIdType.MESH


def split(value):
    hi = value.astype(BF16)
    return hi, (value - hi.astype(F32)).astype(BF16)


class Group:
    def __init__(self, axis, n, part, land, full, note, notes, send, recv, tell_send, tell_recv):
        self.axis, self.n = axis, n
        self.part, self.land, self.full, self.note, self.notes = part, land, full, note, notes
        self.send, self.recv = send, recv
        self.tell_send, self.tell_recv = tell_send, tell_recv
        self.me = lax.axis_index(axis)
        self.count, self.paths, self.width = part.shape

    @staticmethod
    def shape(n, length):
        return (n, n - 1, length // n)

    def peer(self, o):
        return lax.rem(self.me + 1 + o, self.n)

    def copy(self, kind, o, src, dst, peer):
        return pltpu.make_async_remote_copy(
            src_ref=src,
            dst_ref=dst,
            send_sem=self.send.at[kind, o],
            recv_sem=self.recv.at[kind, o],
            device_id={self.axis: peer},
            device_id_type=MESH,
        )

    def scatter(self, o):
        peer = self.peer(o)
        return self.copy(0, o, self.part.at[peer], self.land.at[0, o], peer)

    def gather(self, o):
        return self.copy(1, o, self.full.at[self.me], self.full.at[self.me], self.peer(o))

    def tell(self, turn, o):
        return pltpu.make_async_remote_copy(
            src_ref=self.note.at[turn],
            dst_ref=self.notes.at[turn, o],
            send_sem=self.tell_send.at[turn, o],
            recv_sem=self.tell_recv.at[turn, o],
            device_id={self.axis: self.peer(o)},
            device_id_type=MESH,
        )

    def start_notes(self, turn, *values):
        for i, value in enumerate(values):
            self.note[turn, i : i + 1, :] = value
        for o in range(self.n - 1):
            self.tell(turn, o).start()

    def finish_notes(self, turn):
        for o in range(self.n - 1):
            self.tell(turn, o).wait()
        total = jnp.zeros(self.note.shape[1:], F32)
        for d in range(self.n):
            term = self.note[turn]
            for o in range(self.n - 1):
                term = jnp.where(self.peer(self.n - 2 - o) == d, self.notes[turn, o], term)
            total = total + term
        return total

    def product(self, both, hi_ref, lo_ref, owner):
        paths, step = self.paths, min(CHUNK, self.width)
        for t in range(self.width // step):
            cols = pl.ds(pl.multiple_of(owner * self.width + t * step, 128), step)
            wide = jnp.dot(both[...], hi_ref[:, cols], preferred_element_type=F32)
            low = jnp.dot(both[0:paths, :], lo_ref[:, cols], preferred_element_type=F32)
            self.part[owner, :, t * step : (t + 1) * step] = wide[:paths] + wide[paths:] + low

    def multiply(self, both, hi_ref, lo_ref, between=None):
        def chunk(o, carry):
            self.product(both, hi_ref, lo_ref, self.peer(o))

            @pl.when(o < self.n - 1)
            def _():
                self.scatter(o).start()

            return carry

        lax.fori_loop(0, self.n, chunk, 0)
        if between is not None:
            between()

    def finish_sum(self):
        total = self.part[self.me]
        for o in range(self.n - 1):
            self.scatter(o).wait_recv()
            total = total + self.land[0, o]
        self.full[self.me] = total
        for o in range(self.n - 1):
            self.gather(o).start()
        for o in range(self.n - 1):
            self.scatter(o).wait_send()
        for o in range(self.n - 1):
            self.gather(o).wait()


class Pairs(Group):
    @staticmethod
    def shape(n, length):
        return (length // CHUNK, length // CHUNK, CHUNK)

    def partner(self):
        return self.me + 1 - 2 * lax.rem(self.me, 2)

    def near(self, o, src):
        return self.copy(0, o, self.part.at[src], self.land.at[0, o], self.partner())

    def far(self, o, src):
        return self.copy(1, o, self.part.at[src], self.land.at[1, o], self.across())

    def back(self, o, src):
        return self.copy(2, o, self.full.at[src], self.full.at[src], self.partner())


class Square(Pairs):
    def across(self):
        return lax.rem(self.me + 2, 4)

    def multiply(self, both, hi_ref, lo_ref, between=None):
        half = self.count // 2
        core = lax.rem(self.me, 2)
        mine, other = core * half, (1 - core) * half

        def give(o, carry):
            self.product(both, hi_ref, lo_ref, other + o)
            self.near(o, other + o).start()
            return carry

        def keep(o, carry):
            self.product(both, hi_ref, lo_ref, mine + o)
            self.near(o, other + o).wait_recv()
            self.part[mine + o] += self.land[0, o]
            self.far(o, mine + o).start()
            return carry

        lax.fori_loop(0, half, give, 0)
        if between is not None:
            between()
        lax.fori_loop(0, half, keep, 0)

    def finish_sum(self):
        half = self.count // 2
        core = lax.rem(self.me, 2)
        mine, other = core * half, (1 - core) * half

        def total(o, carry):
            self.far(o, mine + o).wait_recv()
            self.full[mine + o] = self.part[mine + o] + self.land[1, o]
            self.back(o, mine + o).start()
            return carry

        def settle(o, carry):
            self.near(o, other + o).wait_send()
            self.far(o, mine + o).wait_send()
            self.back(o, mine + o).wait()
            return carry

        lax.fori_loop(0, half, total, 0)
        lax.fori_loop(0, half, settle, 0)


class Chain(Pairs):
    def across(self):
        return 3 - self.me

    def inner(self):
        return jnp.logical_or(self.me == 1, self.me == 2)

    def multiply(self, both, hi_ref, lo_ref, between=None):
        def chunk(o, carry):
            self.product(both, hi_ref, lo_ref, o)

            @pl.when(jnp.logical_not(self.inner()))
            def _():
                self.near(o, o).start()

            return carry

        lax.fori_loop(0, self.count, chunk, 0)
        if between is not None:
            between()

    def finish_sum(self):
        count = self.count

        @pl.when(self.inner())
        def _():
            def relay(o, carry):
                @pl.when(o < count)
                def _():
                    self.near(o, o).wait_recv()
                    self.part[o] += self.land[0, o]
                    self.far(o, o).start()

                @pl.when(o >= LAG)
                def _():
                    p = o - LAG
                    self.far(p, p).wait_recv()
                    self.full[p] = self.part[p] + self.land[1, p]
                    self.back(p, p).start()

                return carry

            def settle(o, carry):
                self.far(o, o).wait_send()
                self.back(o, o).wait_send()
                return carry

            lax.fori_loop(0, count + LAG, relay, 0)
            lax.fori_loop(0, count, settle, 0)

        @pl.when(jnp.logical_not(self.inner()))
        def _():
            def settle(o, carry):
                self.near(o, o).wait_send()
                self.back(o, o).wait_recv()
                return carry

            lax.fori_loop(0, count, settle, 0)


def col_kind(n):
    return Square if n == 4 else Group


def row_kind(n):
    return Chain if n == 4 else Group


def kernel(
    nc, nr, matrix, sign, lambdas, x_prev, w_prev, p_prev, z_prev, u_prev,
    coeffs, sparse, margins, mdual,
    a_hi, a_lo, t_hi, t_lo, stage, stage_sem, both_f, both_s,
    dual, resid, direction, image_of, mapped, scal,
    *comm,
):
    cols = col_kind(nc)("cols", nc, *comm[:9])
    rows = row_kind(nr)("rows", nr, *comm[9:])
    samples, features = matrix.shape
    paths = x_prev.shape[0]
    blocks = samples // TILE

    barrier = pltpu.get_barrier_semaphore()
    for group in (cols, rows):
        for o in range(group.n - 1):
            pl.semaphore_signal(
                barrier, inc=1, device_id={group.axis: group.peer(o)}, device_id_type=MESH
            )

    def load(i, slot):
        return pltpu.make_async_copy(
            matrix.at[pl.ds(pl.multiple_of(i * TILE, TILE), TILE)], stage.at[slot], stage_sem.at[slot]
        )

    load(0, 0).start()
    coeffs[...] = x_prev[...]
    sparse[...] = w_prev[...]
    dual[...] = p_prev[...]
    margins[...] = z_prev[...]
    mdual[...] = u_prev[...]
    resid[...] = x_prev[...]
    direction[...] = jnp.zeros_like(direction)
    mapped[...] = jnp.zeros_like(mapped)
    image_of[...] = jnp.zeros_like(image_of)
    scal[...] = jnp.ones_like(scal)
    cols.note[...] = jnp.zeros_like(cols.note)
    rows.note[...] = jnp.zeros_like(rows.note)
    lane = lax.broadcasted_iota(jnp.int32, (paths, 128), 1)
    diagonal = lane == lax.broadcasted_iota(jnp.int32, (paths, 128), 0)

    def prepare(i, carry):
        slot = lax.rem(i, 2)
        load(i, slot).wait()

        @pl.when(i + 1 < blocks)
        def _():
            load(i + 1, 1 - slot).start()

        down = pl.ds(pl.multiple_of(i * TILE, TILE), TILE)

        def block(j, carry):
            across = pl.ds(pl.multiple_of(j * TILE, TILE), TILE)
            value = stage[slot, :, across]
            a_hi[down, across], a_lo[down, across] = split(value)
            t_hi[across, down], t_lo[across, down] = split(value.T)
            return carry

        return lax.fori_loop(0, features // TILE, block, carry, unroll=2)

    lax.fori_loop(0, blocks, prepare, 0)
    pl.semaphore_wait(barrier, cols.n + rows.n - 2)

    def spread(value):
        return jnp.broadcast_to(value, (paths, 128))

    def rowsum(value):
        value = jnp.sum(value, axis=1, keepdims=True)
        return jnp.sum(jnp.where(diagonal, value, 0.0), axis=0, keepdims=True)

    def per_path(row):
        return spread(jnp.sum(jnp.where(diagonal, row, 0.0), axis=1, keepdims=True))

    def advance(alpha):
        coeffs[...] += alpha * direction[...]
        image_of[...] += alpha * mapped[...]

    def proximal():
        piece = min(1024, samples)
        for c in range(samples // piece):
            at = slice(c * piece, (c + 1) * piece)
            target = image_of[:, at] + mdual[:, at]
            sgn = sign[:, at]

            def newton(_, m):
                s = 1.0 / (1.0 + jnp.exp(sgn * m))
                return m - (m - target - sgn * s) / (1.0 + s * (1.0 - s))

            m = lax.fori_loop(0, NEWTON_STEPS, newton, target)
            margins[:, at] = m
            mdual[:, at] = target - m
        total = coeffs[...] + dual[...]
        lam = lambdas[...]
        clipped = jnp.minimum(jnp.maximum(total, -lam), lam)
        sparse[...] = total - clipped
        dual[...] = clipped

    last = ITERS * CG_STEPS

    def pair(k, carry):
        step = lax.rem(k + CG_STEPS - 1, CG_STEPS)
        first = jnp.logical_or(step == 0, k == 0)
        closing = jnp.logical_or(step == CG_STEPS - 1, k == 0)
        r = resid[...]
        both_f[0:paths, :], both_f[paths:, :] = split(r)
        rr, rd = rowsum(r * r), rowsum(r * direction[...])
        turn = lax.rem(k, 2)
        cols.start_notes(turn, rr, rd)

        def direction_step():
            notes = cols.finish_notes(turn)
            rr, rd = per_path(notes[0:1]), per_path(notes[1:2])
            beta = jnp.where(first, 0.0, rr / scal[0])
            scal[1] = rr + 2.0 * beta * rd + beta * beta * scal[1]
            scal[0] = rr
            scal[2] = beta

            @pl.when(k > 0)
            def _():
                direction[...] = resid[...] + beta[:, 0:1] * direction[...]

        cols.multiply(both_f, t_hi, t_lo, direction_step)
        cols.finish_sum()

        @pl.when(k == 0)
        def _():
            for c in range(cols.count):
                image_of[:, c * cols.width : (c + 1) * cols.width] = cols.full[c]

        @pl.when(k > 0)
        def _():
            beta = scal[2][:, 0:1]
            for c in range(cols.count):
                at = slice(c * cols.width, (c + 1) * cols.width)
                mapped[:, at] = cols.full[c] + beta * mapped[:, at]

        m = mapped[...]
        rows.start_notes(turn, rowsum(m * m))

        @pl.when(closing)
        def _():
            @pl.when(k > 0)
            def _():
                sq = per_path(rows.finish_notes(turn)[0:1])
                advance((scal[0] / (scal[1] + sq))[:, 0:1])
                proximal()
                direction[...] = jnp.zeros_like(direction)
                mapped[...] = jnp.zeros_like(mapped)

            @pl.when(k == 0)
            def _():
                rows.finish_notes(turn)

            both_s[0:paths, :], both_s[paths:, :] = split(margins[...] - mdual[...] - image_of[...])

        @pl.when(jnp.logical_not(closing))
        def _():
            both_s[0:paths, :], both_s[paths:, :] = split(m)

        @pl.when(k < last)
        def _():
            def length_step():
                @pl.when(jnp.logical_not(closing))
                def _():
                    sq = per_path(rows.finish_notes(turn)[0:1])
                    alpha = scal[0] / (scal[1] + sq)
                    scal[2] = alpha
                    advance(alpha[:, 0:1])

            rows.multiply(both_s, a_hi, a_lo, length_step)
            rows.finish_sum()

            @pl.when(closing)
            def _():
                for c in range(rows.count):
                    at = slice(c * rows.width, (c + 1) * rows.width)
                    resid[:, at] = sparse[:, at] - dual[:, at] - coeffs[:, at] + rows.full[c]

            @pl.when(jnp.logical_not(closing))
            def _():
                alpha = scal[2][:, 0:1]
                for c in range(rows.count):
                    at = slice(c * rows.width, (c + 1) * rows.width)
                    resid[:, at] = resid[:, at] - alpha * (direction[:, at] + rows.full[c])

        return carry

    lax.fori_loop(0, last + 1, pair, 0)


def local(nc, nr, matrix, labels, lambdas, x_prev, w_prev, p_prev, z_prev, u_prev):
    sign = (2.0 * labels.astype(F32) - 1.0)[None, :]
    samples, features = matrix.shape
    paths = x_prev.shape[0]
    fvec, svec = (paths, features), (paths, samples)

    def comm(kind, n, length):
        count, slots, width = kind.shape(n, length)
        return [
            pltpu.VMEM((count, paths, width), F32),
            pltpu.VMEM((2, slots, paths, width), F32),
            pltpu.VMEM((count, paths, width), F32),
            pltpu.VMEM((2, 8, 128), F32),
            pltpu.VMEM((2, n - 1, 8, 128), F32),
            pltpu.SemaphoreType.DMA((3, slots)),
            pltpu.SemaphoreType.DMA((3, slots)),
            pltpu.SemaphoreType.DMA((2, n - 1)),
            pltpu.SemaphoreType.DMA((2, n - 1)),
        ]

    vmem = pl.BlockSpec(memory_space=pltpu.VMEM)
    return pl.pallas_call(
        functools.partial(kernel, nc, nr),
        out_shape=tuple(jax.ShapeDtypeStruct(s, F32) for s in (fvec, fvec, svec, svec)),
        in_specs=[pl.BlockSpec(memory_space=pl.ANY)] + [vmem] * 7,
        out_specs=(vmem,) * 4,
        scratch_shapes=[
            pltpu.VMEM((samples, features), BF16),
            pltpu.VMEM((samples, features), BF16),
            pltpu.VMEM((features, samples), BF16),
            pltpu.VMEM((features, samples), BF16),
            pltpu.VMEM((2, TILE, features), F32),
            pltpu.SemaphoreType.DMA((2,)),
            pltpu.VMEM((2 * paths, features), BF16),
            pltpu.VMEM((2 * paths, samples), BF16),
            pltpu.VMEM(fvec, F32),
            pltpu.VMEM(fvec, F32),
            pltpu.VMEM(fvec, F32),
            pltpu.VMEM(svec, F32),
            pltpu.VMEM(svec, F32),
            pltpu.VMEM((3, paths, 128), F32),
        ]
        + comm(col_kind(nc), nc, samples)
        + comm(row_kind(nr), nr, features),
        compiler_params=pltpu.CompilerParams(
            collective_id=0, has_side_effects=True, vmem_limit_bytes=60 * 1024 * 1024
        ),
    )(matrix, sign, lambdas[:, None], x_prev, w_prev, p_prev, z_prev, u_prev)


def solution(mesh):
    return jax.shard_map(
        functools.partial(local, mesh.shape["cols"], mesh.shape["rows"]),
        mesh=mesh,
        in_specs=(
            P(("rep", "rows"), "cols"),
            P(("rep", "rows")),
            P("rep"),
            P("rep", "cols"),
            P("rep", "cols"),
            P("rep", "cols"),
            P("rep", "rows"),
            P("rep", "rows"),
        ),
        out_specs=(P("rep", "cols"), P("rep", "cols"), P("rep", "rows"), P("rep", "rows")),
        check_vma=False,
    )
```
